32 devices in a mesh: dimer: 8 (over z, x), rep: 4 (over y, core).
Axes of the slice: x: 2, y: 2, z: 4, core: 2. Of those that a mesh axis runs over, the one named last changes fastest.
Arguments:
- integrals: bfloat16 [256, 256, 3, 128], P('dimer', 'rep'), may hold values from -0.375 to 0.375
- density: bfloat16 [256, 256], P('dimer', 'rep'), may hold values from -6 to 6
- energy_terms: bfloat16 [256, 256], P('dimer', 'rep'), may hold values from -0.0234375 to 0.0234375
- positions: float32 [3, 16384], P(None, ('dimer', 'rep')), may hold values from -0.046875 to 0.046875
- dimer_owners: int32 [256, 2], P('dimer'), may hold values from 0 to 7, all different within a row; in each aligned block of 32 rows (0 to 31, 32 to 63, ...) at most 16 rows name the same one
- dimer_local: int32 [256, 2], P('dimer'), may hold values from 0 to 31
Outputs:
- forces: float32 [3, 16384], P(None, ('dimer', 'rep'))
- energy: float32 [], replicated
- virial: float32 [], replicated
The draws below stay inside these ranges and needn't reach their ends.
Inputs may be any that keep to these rules, and one draw needn't show every extreme that they name: `dimer_owners`: the two entries of a row differ. Among the 32 rows of one device no value stands more than 16 times, and some value stands exactly 16 times in some device's rows.
All inputs are finite; a program needn't handle non-finite values.
Results may differ from the reference program's by a relative error of at most 0.00045.
Values sent between devices are 32-bit elements; how exact they have to be, the bound alone decides.
A program may use at most 64 MiB of HBM per device.

```python
import math
import jax
import jax.numpy as jnp
import numpy as np
from jax import lax

A = 64
NTERMS = 256
FRAG_DEV = 32
DIM_DEV = 32
OWNERS = 8
FRAGMENTS = 256
ATOMS = 16384
DIMERS = 256
CAP = 16


def plant(result, stream_key, least, largest):
    extent = result.shape
    place = [jax.random.randint(jax.random.fold_in(stream_key, axis), (), 0, extent[axis]) for axis in range(len(extent))]
    result = result.at[tuple(place)].set(least)
    longest = extent.index(max(extent))
    place[longest] = (place[longest] + 1) % extent[longest]
    return result.at[tuple(place)].set(largest)


def steps_of(own_key, dims, shards, smallest, high):
    factor_of, own = 1.0, jax.random.fold_in(own_key, 6)
    for position, blocks in shards:
        draws = jnp.exp(jax.random.uniform(jax.random.fold_in(own, position), (blocks,), jnp.float32, smallest / len(shards), high / len(shards)))
        factor_of = factor_of * jnp.repeat(draws, dims[position] // blocks).reshape([-1 if axis == position else 1 for axis in range(len(dims))])
    return factor_of


def deal_out(stream_key, own, number, rows, amount, top, most, lean):
    order = jax.random.permutation(stream_key, amount)
    packed, usual = portions_of(amount, rows * top, most, lean, True), portions_of(amount, rows * top, most, lean, False)
    places = jnp.arange(amount)

    def named(tallies, rotation):
        used = int((tallies > 0).sum())
        fixed = max(1, used // 4)
        passed = fixed + (places - fixed + rotation * (used - fixed)) % max(1, amount - fixed)
        return jnp.zeros((amount,), jnp.int32).at[order[jnp.where(places < fixed, places, passed)]].set(jnp.asarray(tallies, jnp.int32))

    tallies = jnp.where(number % 4 == 0, named(packed, number // 4), named(usual, number - number // 4 - 1))
    mixed = jax.random.permutation(jax.random.fold_in(own, 3), amount)
    donor, taker = mixed[0:amount // 2 * 2:2], mixed[1:amount // 2 * 2:2]
    slack = jnp.minimum(tallies[donor] - 1, most - tallies[taker]) // 2
    slack = jnp.where((donor == order[0]) | (taker == order[0]) | (tallies[taker] == 0), 0, jnp.maximum(slack, 0))
    passed = jax.random.randint(jax.random.fold_in(own, 4), (amount // 2,), 0, 1 << 20) % (slack + 1)
    tallies = tallies.at[donor].add(-passed).at[taker].add(passed)
    labels = jnp.searchsorted(jnp.cumsum(tallies), jnp.arange(rows * top), side="right").astype(jnp.int32)
    grid = labels.reshape(top, rows).T
    grid = grid[jax.random.permutation(jax.random.fold_in(own, 1), rows)]
    rotation = jax.random.randint(jax.random.fold_in(own, 2), (rows, 1), 0, top)
    return jnp.take_along_axis(grid, (jnp.arange(top)[None, :] + rotation) % top, axis=1)


def portions_of(amount, total, most, slope, full):
    weights = [(1 << 20) // math.isqrt(rank ** slope) + 1 for rank in range(1, amount + 1)]
    largest = most if full else min(most, max(-(-total // amount), total * weights[0] // sum(weights)))
    least = 1 if total - largest >= amount - 1 else 0
    given, surplus = [largest] + [least] * (amount - 1), total - largest - least * (amount - 1)
    while surplus > 0:
        free = [i for i in range(1, amount) if given[i] < largest] or [i for i in range(1, amount) if given[i] < most]
        pool, budget = sum([weights[i] for i in free]), surplus
        for i in free:
            extra = min(most - given[i], max(1, budget * weights[i] // pool), surplus)
            given[i] = given[i] + extra
            surplus = surplus - extra
    return np.array(given)


def normal_values(stream_key, shape, scale, most, cuts=(), kind=jnp.bfloat16):
    values = scale * jax.random.normal(stream_key, shape, jnp.float32)
    if cuts:
        values = values * steps_of(stream_key, shape, cuts, -0.22, 0.18)
    return jnp.clip(values, -most, most).astype(kind)


def setup_inputs(seed: int = 0) -> dict:
    key_of = jax.random.split(jax.random.key(seed), 7)
    integrals = normal_values(key_of[0], (DIMERS, NTERMS, 3, 2 * A), NTERMS ** -0.5, 0.375, ((0, 8), (1, 4)))
    density = normal_values(key_of[1], (DIMERS, NTERMS), 1.0, 6.0, ((0, 8), (1, 4)))
    energy_terms = normal_values(key_of[2], (DIMERS, NTERMS), (NTERMS * DIMERS) ** -0.5, 0.0234375, ((0, 8), (1, 4)))
    positions = normal_values(key_of[3], (3, ATOMS), (ATOMS ** -0.5), 0.046875, ((1, 32),), jnp.float32)
    dimer_owners_keys = jax.random.split(jax.random.fold_in(key_of[4], 1), DIMERS // DIM_DEV)
    dimer_owners_turns = jax.random.permutation(jax.random.fold_in(key_of[4], 3), DIMERS // DIM_DEV)
    dimer_owners = jax.vmap(lambda own, number: deal_out(jax.random.fold_in(key_of[4], 2), own, number, DIM_DEV, OWNERS, 2, CAP, 2))(dimer_owners_keys, dimer_owners_turns).reshape((DIMERS, 2))
    dimer_local = plant(jax.random.randint(key_of[5], (DIMERS, 2), 0, FRAG_DEV), jax.random.fold_in(key_of[5], 1), 0, FRAG_DEV - 1).astype(jnp.int32)
    return dict(integrals=integrals, density=density, energy_terms=energy_terms, positions=positions, dimer_owners=dimer_owners, dimer_local=dimer_local)


def contract(block):
    weights, ints = block
    return jnp.einsum("sk,skcb->scb", weights.astype(jnp.float32), ints.astype(jnp.float32))


def reference(integrals, density, energy_terms, positions, dimer_owners, dimer_local):
    grads = lax.map(contract, (density.reshape(OWNERS, DIM_DEV, NTERMS), integrals.reshape(OWNERS, DIM_DEV, NTERMS, 3, 2 * A)))
    grads = grads.reshape(DIMERS, 3, 2, A)
    pieces = jnp.transpose(grads, (0, 2, 1, 3)).reshape(DIMERS * 2, 3, A)
    fragment = (dimer_owners * FRAG_DEV + dimer_local).reshape(-1).astype(jnp.int32)
    summed = jax.ops.segment_sum(pieces, fragment, num_segments=FRAGMENTS)
    forces = jnp.transpose(summed, (1, 0, 2)).reshape(3, ATOMS)
    energy = jnp.sum(density.astype(jnp.float32) * energy_terms.astype(jnp.float32))
    virial = -jnp.sum(positions * forces) / 3.0
    return forces, energy, virial
```

```python
import functools

import jax
import jax.numpy as jnp
from jax import lax
from jax.experimental import pallas as pl
from jax.experimental.pallas import tpu as pltpu
from jax.sharding import PartitionSpec as P

MESH = pl.DeviceIdType.MESH
F32, BF16 = jnp.float32, jnp.bfloat16


def kernel(
    n_d, n_r, integ, dens, eterm, pos, owner, local, forces, scalars,
    ibuf, dbuf, in_a, acc, in_b, posb, in_p, sbuf, in_s,
    isem, a_send, a_recv, b_send, b_recv, p_send, p_recv, s_send, s_recv,
):
    slots, terms = dens.shape
    lanes = ibuf.shape[3]
    half = lanes // 2
    pairs = pos.shape[1] // lanes
    per_rep = 2 * pairs
    n_all = n_d * n_r
    rows = n_r * n_d * pairs
    d, r = lax.axis_index("dimer"), lax.axis_index("rep")
    me = d * n_r + r

    def device(step):
        peer = lax.rem(me + step, n_all)
        return (peer // n_r, lax.rem(peer, n_r))

    loads = [pltpu.make_async_copy(integ.at[:, c], ibuf.at[c], isem.at[c]) for c in range(3)]
    for load in loads:
        load.start()

    barrier = pltpu.get_barrier_semaphore()

    def greet(step, carry):
        pl.semaphore_signal(barrier, inc=1, device_id=device(step), device_id_type=MESH)
        return carry

    lax.fori_loop(1, n_all, greet, 0)

    weights = dens[...].astype(F32)
    span = slots * terms
    lane = lax.broadcasted_iota(jnp.int32, (slots, span), 1)
    first = lax.broadcasted_iota(jnp.int32, (slots, span), 0) * terms
    spread = jnp.concatenate([weights] * slots, axis=1)
    diagonal = jnp.where((lane >= first) & (lane < first + terms), spread, 0.0).astype(BF16)

    name, index = owner[...], local[...]
    rep = jnp.zeros_like(index)
    for bound in range(1, n_r):
        rep = rep + (index >= bound * per_rep).astype(jnp.int32)
    rest = index - rep * per_rep
    target = rep * (n_d * pairs) + name * pairs + lax.shift_right_logical(rest, 1)
    parity = rest & 1
    keys = []
    for t in range(2):
        for h in range(2):
            keys.append(jnp.where(parity[t : t + 1] == h, target[t : t + 1], -1))
    key = jnp.concatenate(keys, axis=1)
    place = lax.broadcasted_iota(jnp.int32, (rows, 4 * slots), 0)
    hot = jnp.where(place == key, 1.0, 0.0).astype(BF16)
    hot = jnp.concatenate([hot] * 3, axis=1)

    for c in range(3):
        for j in range(pairs):
            posb[c * pairs + j : c * pairs + j + 1] = pos[c : c + 1, j * lanes : (j + 1) * lanes]
    energy = jnp.sum(weights * eterm[...].astype(F32), axis=0, keepdims=True)
    sbuf[1:2] = jnp.concatenate([energy, jnp.zeros((1, lanes - terms), F32)], axis=1)

    side = lax.broadcasted_iota(jnp.int32, (slots, lanes), 1) >= half
    for c in range(3):
        loads[c].wait()
        grad = jnp.dot(
            diagonal, ibuf[c].reshape(span, lanes), preferred_element_type=F32
        )
        swap = pltpu.roll(grad, half, 1)
        spreads = jnp.concatenate(
            [
                jnp.where(side, 0.0, grad),
                jnp.where(side, swap, 0.0),
                jnp.where(side, 0.0, swap),
                jnp.where(side, grad, 0.0),
            ],
            axis=0,
        )
        high = spreads.astype(BF16)
        left = spreads - high.astype(F32)
        middle = left.astype(BF16)
        low = (left - middle.astype(F32)).astype(BF16)
        placed = jnp.dot(
            hot, jnp.concatenate([high, middle, low], axis=0), preferred_element_type=F32
        )
        for q in range(n_r):
            dbuf[q, c] = placed[q * n_d * pairs : (q + 1) * n_d * pairs]

    pl.semaphore_wait(barrier, n_all - 1)

    a_copies = []
    for k in range(1, n_r):
        to = lax.rem(r + k, n_r)
        a_copies.append(
            pltpu.make_async_remote_copy(
                src_ref=dbuf.at[to], dst_ref=in_a.at[k - 1],
                send_sem=a_send.at[k - 1], recv_sem=a_recv.at[k - 1],
                device_id=(d, to), device_id_type=MESH,
            )
        )
    for copy in a_copies:
        copy.start()

    def p_copy(k):
        return pltpu.make_async_remote_copy(
            src_ref=posb, dst_ref=in_p.at[k - 1],
            send_sem=p_send.at[k - 1], recv_sem=p_recv.at[k - 1],
            device_id=(lax.rem(d + k, n_d), r), device_id_type=MESH,
        )

    def b_copy(k):
        to = lax.rem(d + k, n_d)
        return pltpu.make_async_remote_copy(
            src_ref=acc.at[to], dst_ref=in_b.at[k - 1],
            send_sem=b_send.at[k - 1], recv_sem=b_recv.at[k - 1],
            device_id=(to, r), device_id_type=MESH,
        )

    def s_copy(k):
        return pltpu.make_async_remote_copy(
            src_ref=sbuf, dst_ref=in_s.at[k - 1],
            send_sem=s_send.at[k - 1], recv_sem=s_recv.at[k - 1],
            device_id=device(k), device_id_type=MESH,
        )

    def each(last, act):
        def body(k, carry):
            act(k)
            return carry

        lax.fori_loop(1, last, body, 0)

    each(n_d, lambda k: p_copy(k).start())
    for copy in a_copies:
        copy.wait_recv()
    for c in range(3):
        total = dbuf[r, c]
        for k in range(n_r - 1):
            total = total + in_a[k, c]
        for o in range(n_d):
            acc[o, c * pairs : (c + 1) * pairs] = total[o * pairs : (o + 1) * pairs]
    each(n_d, lambda k: b_copy(k).start())
    each(n_d, lambda k: p_copy(k).wait_recv())

    def virial_of(k, carry):
        return carry + acc[lax.rem(d - k + n_d, n_d)] * in_p[k - 1]

    products = lax.fori_loop(1, n_d, virial_of, acc[d] * posb[...])
    sbuf[0:1] = jnp.sum(products, axis=0, keepdims=True)
    each(n_all, lambda k: s_copy(k).start())

    each(n_d, lambda k: b_copy(k).wait_recv())
    total = lax.fori_loop(1, n_d, lambda k, carry: carry + in_b[k - 1], acc[d])
    for c in range(3):
        for j in range(pairs):
            forces[c : c + 1, j * lanes : (j + 1) * lanes] = total[c * pairs + j : c * pairs + j + 1]

    each(n_all, lambda k: s_copy(k).wait_recv())
    both = lax.fori_loop(1, n_all, lambda k, carry: carry + in_s[k - 1], sbuf[...])
    both = jnp.sum(both, axis=1, keepdims=True)
    row = lax.broadcasted_iota(jnp.int32, both.shape, 0)
    both = jnp.where(row == 0, both / -3.0, both)
    scalars[...] = jnp.broadcast_to(both, scalars.shape)

    for copy in a_copies:
        copy.wait_send()
    each(n_d, lambda k: p_copy(k).wait_send())
    each(n_d, lambda k: b_copy(k).wait_send())
    each(n_all, lambda k: s_copy(k).wait_send())


def on_device(n_d, n_r, integrals, density, energy_terms, positions, owners, local):
    slots, terms, _, lanes = integrals.shape
    pairs = positions.shape[1] // lanes
    n_all = n_d * n_r
    vmem = pl.BlockSpec(memory_space=pltpu.VMEM)
    dma = pltpu.SemaphoreType.DMA
    forces, scalars = pl.pallas_call(
        functools.partial(kernel, n_d, n_r),
        out_shape=(
            jax.ShapeDtypeStruct(positions.shape, F32),
            jax.ShapeDtypeStruct((2, lanes), F32),
        ),
        in_specs=[pl.BlockSpec(memory_space=pl.ANY)] + [vmem] * 5,
        out_specs=(vmem, vmem),
        scratch_shapes=[
            pltpu.VMEM((3, slots, terms, lanes), BF16),
            pltpu.VMEM((n_r, 3, n_d * pairs, lanes), F32),
            pltpu.VMEM((n_r - 1, 3, n_d * pairs, lanes), F32),
            pltpu.VMEM((n_d, 3 * pairs, lanes), F32),
            pltpu.VMEM((n_d - 1, 3 * pairs, lanes), F32),
            pltpu.VMEM((3 * pairs, lanes), F32),
            pltpu.VMEM((n_d - 1, 3 * pairs, lanes), F32),
            pltpu.VMEM((2, lanes), F32),
            pltpu.VMEM((n_all - 1, 2, lanes), F32),
            dma((3,)),
            dma((n_r - 1,)), dma((n_r - 1,)),
            dma((n_d - 1,)), dma((n_d - 1,)),
            dma((n_d - 1,)), dma((n_d - 1,)),
            dma((n_all - 1,)), dma((n_all - 1,)),
        ],
        compiler_params=pltpu.CompilerParams(collective_id=0, has_side_effects=True),
    )(
        jnp.transpose(integrals, (0, 2, 1, 3)), density, energy_terms, positions,
        owners.T, local.T,
    )
    return forces, scalars[1, 0], scalars[0, 0]


def solution(mesh):
    in_specs = (
        P("dimer", "rep", None, None),
        P("dimer", "rep"),
        P("dimer", "rep"),
        P(None, ("dimer", "rep")),
        P("dimer", None),
        P("dimer", None),
    )
    out_specs = (P(None, ("dimer", "rep")), P(), P())
    return jax.shard_map(
        functools.partial(on_device, mesh.shape["dimer"], mesh.shape["rep"]),
        mesh=mesh, in_specs=in_specs, out_specs=out_specs, check_vma=False,
    )
```

```python
import functools

import jax
import jax.numpy as jnp
from jax import lax
from jax.experimental import pallas as pl
from jax.experimental.pallas import tpu as pltpu
from jax.sharding import PartitionSpec as P

MESH = pl.DeviceIdType.MESH
F32, BF16 = jnp.float32, jnp.bfloat16


def kernel(
    n_d, n_r, integ, *refs,
):
    smalls, (forces, scalars), (dens, eterm, pos, owner, local) = refs[:5], refs[5:7], refs[7:12]
    (
        ibuf, dbuf, in_a, acc, in_b, posb, in_p, sbuf, in_s,
        isem, a_send, a_recv, b_send, b_recv, p_send, p_recv, s_send, s_recv,
    ) = refs[12:]
    slots, terms = dens.shape
    lanes = ibuf.shape[3]
    half = lanes // 2
    pairs = pos.shape[1] // lanes
    per_rep = 2 * pairs
    n_all = n_d * n_r
    rows = n_r * n_d * pairs
    d, r = lax.axis_index("dimer"), lax.axis_index("rep")
    me = d * n_r + r

    def device(step):
        peer = lax.rem(me + step, n_all)
        return (peer // n_r, lax.rem(peer, n_r))

    loads = [pltpu.make_async_copy(integ.at[:, c], ibuf.at[c], isem.at[c]) for c in range(3)]
    fetches = [
        pltpu.make_async_copy(source, held, isem.at[3 + i])
        for i, (source, held) in enumerate(zip(smalls, (dens, eterm, pos, owner, local)))
    ]
    for copy in loads + fetches:
        copy.start()

    barrier = pltpu.get_barrier_semaphore()

    def greet(step, carry):
        pl.semaphore_signal(barrier, inc=1, device_id=device(step), device_id_type=MESH)
        return carry

    lax.fori_loop(1, n_all, greet, 0)

    for fetch in fetches:
        fetch.wait()

    weights = dens[...].astype(F32)
    span = slots * terms
    lane = lax.broadcasted_iota(jnp.int32, (slots, span), 1)
    first = lax.broadcasted_iota(jnp.int32, (slots, span), 0) * terms
    spread = jnp.concatenate([weights] * slots, axis=1)
    diagonal = jnp.where((lane >= first) & (lane < first + terms), spread, 0.0).astype(BF16)

    name, index = owner[...], local[...]
    rep = jnp.zeros_like(index)
    for bound in range(1, n_r):
        rep = rep + (index >= bound * per_rep).astype(jnp.int32)
    rest = index - rep * per_rep
    target = rep * (n_d * pairs) + name * pairs + lax.shift_right_logical(rest, 1)
    parity = rest & 1
    keys = []
    for t in range(2):
        for h in range(2):
            keys.append(jnp.where(parity[t : t + 1] == h, target[t : t + 1], -1))
    key = jnp.concatenate(keys, axis=1)
    place = lax.broadcasted_iota(jnp.int32, (rows, 4 * slots), 0)
    hot = jnp.where(place == key, 1.0, 0.0).astype(BF16)
    hot = jnp.concatenate([hot] * 3, axis=1)

    for c in range(3):
        for j in range(pairs):
            posb[c * pairs + j : c * pairs + j + 1] = pos[c : c + 1, j * lanes : (j + 1) * lanes]
    energy = jnp.sum(weights * eterm[...].astype(F32), axis=0, keepdims=True)
    sbuf[1:2] = jnp.concatenate([energy, jnp.zeros((1, lanes - terms), F32)], axis=1)

    side = lax.broadcasted_iota(jnp.int32, (slots, lanes), 1) >= half
    for c in range(3):
        loads[c].wait()
        grad = jnp.dot(
            diagonal, ibuf[c].reshape(span, lanes), preferred_element_type=F32
        )
        swap = pltpu.roll(grad, half, 1)
        spreads = jnp.concatenate(
            [
                jnp.where(side, 0.0, grad),
                jnp.where(side, swap, 0.0),
                jnp.where(side, 0.0, swap),
                jnp.where(side, grad, 0.0),
            ],
            axis=0,
        )
        high = spreads.astype(BF16)
        left = spreads - high.astype(F32)
        middle = left.astype(BF16)
        low = (left - middle.astype(F32)).astype(BF16)
        placed = jnp.dot(
            hot, jnp.concatenate([high, middle, low], axis=0), preferred_element_type=F32
        )
        for q in range(n_r):
            dbuf[q, c] = placed[q * n_d * pairs : (q + 1) * n_d * pairs]

    pl.semaphore_wait(barrier, n_all - 1)

    a_copies = []
    for k in range(1, n_r):
        to = lax.rem(r + k, n_r)
        a_copies.append(
            pltpu.make_async_remote_copy(
                src_ref=dbuf.at[to], dst_ref=in_a.at[k - 1],
                send_sem=a_send.at[k - 1], recv_sem=a_recv.at[k - 1],
                device_id=(d, to), device_id_type=MESH,
            )
        )
    for copy in a_copies:
        copy.start()

    def p_copy(k):
        return pltpu.make_async_remote_copy(
            src_ref=posb, dst_ref=in_p.at[k - 1],
            send_sem=p_send.at[k - 1], recv_sem=p_recv.at[k - 1],
            device_id=(lax.rem(d + k, n_d), r), device_id_type=MESH,
        )

    def b_copy(k):
        to = lax.rem(d + k, n_d)
        return pltpu.make_async_remote_copy(
            src_ref=acc.at[to], dst_ref=in_b.at[k - 1],
            send_sem=b_send.at[k - 1], recv_sem=b_recv.at[k - 1],
            device_id=(to, r), device_id_type=MESH,
        )

    def s_copy(k):
        return pltpu.make_async_remote_copy(
            src_ref=sbuf, dst_ref=in_s.at[k - 1],
            send_sem=s_send.at[k - 1], recv_sem=s_recv.at[k - 1],
            device_id=device(k), device_id_type=MESH,
        )

    def each(last, act):
        def body(k, carry):
            act(k)
            return carry

        lax.fori_loop(1, last, body, 0)

    each(n_d, lambda k: p_copy(k).start())
    for copy in a_copies:
        copy.wait_recv()
    for c in range(3):
        total = dbuf[r, c]
        for k in range(n_r - 1):
            total = total + in_a[k, c]
        for o in range(n_d):
            acc[o, c * pairs : (c + 1) * pairs] = total[o * pairs : (o + 1) * pairs]
    each(n_d, lambda k: b_copy(k).start())
    each(n_d, lambda k: p_copy(k).wait_recv())

    def virial_of(k, carry):
        return carry + acc[lax.rem(d - k + n_d, n_d)] * in_p[k - 1]

    products = lax.fori_loop(1, n_d, virial_of, acc[d] * posb[...])
    sbuf[0:1] = jnp.sum(products, axis=0, keepdims=True)
    each(n_all, lambda k: s_copy(k).start())

    each(n_d, lambda k: b_copy(k).wait_recv())
    total = lax.fori_loop(1, n_d, lambda k, carry: carry + in_b[k - 1], acc[d])
    for c in range(3):
        for j in range(pairs):
            forces[c : c + 1, j * lanes : (j + 1) * lanes] = total[c * pairs + j : c * pairs + j + 1]

    each(n_all, lambda k: s_copy(k).wait_recv())
    both = lax.fori_loop(1, n_all, lambda k, carry: carry + in_s[k - 1], sbuf[...])
    both = jnp.sum(both, axis=1, keepdims=True)
    row = lax.broadcasted_iota(jnp.int32, both.shape, 0)
    both = jnp.where(row == 0, both / -3.0, both)
    scalars[...] = jnp.broadcast_to(both, scalars.shape)

    for copy in a_copies:
        copy.wait_send()
    each(n_d, lambda k: p_copy(k).wait_send())
    each(n_d, lambda k: b_copy(k).wait_send())
    each(n_all, lambda k: s_copy(k).wait_send())


def on_device(n_d, n_r, integrals, density, energy_terms, positions, owners, local):
    slots, terms, _, lanes = integrals.shape
    pairs = positions.shape[1] // lanes
    n_all = n_d * n_r
    room = 2 * (2 * integrals.size + 4 * lanes * 8 * n_d * n_r * (3 * pairs + 4)) + 2**21
    vmem = pl.BlockSpec(memory_space=pltpu.VMEM)
    dma = pltpu.SemaphoreType.DMA
    inputs = (
        jnp.transpose(integrals, (0, 2, 1, 3)), density, energy_terms, positions,
        owners.T, local.T,
    )
    forces, scalars = pl.pallas_call(
        functools.partial(kernel, n_d, n_r),
        out_shape=(
            jax.ShapeDtypeStruct(positions.shape, F32),
            jax.ShapeDtypeStruct((2, lanes), F32),
        ),
        in_specs=[pl.BlockSpec(memory_space=pltpu.HBM)] * 6,
        out_specs=(vmem, vmem),
        scratch_shapes=[
            pltpu.VMEM(density.shape, BF16),
            pltpu.VMEM(energy_terms.shape, BF16),
            pltpu.VMEM(positions.shape, F32),
            pltpu.VMEM((2, slots), jnp.int32),
            pltpu.VMEM((2, slots), jnp.int32),
            pltpu.VMEM((3, slots, terms, lanes), BF16),
            pltpu.VMEM((n_r, 3, n_d * pairs, lanes), F32),
            pltpu.VMEM((n_r - 1, 3, n_d * pairs, lanes), F32),
            pltpu.VMEM((n_d, 3 * pairs, lanes), F32),
            pltpu.VMEM((n_d - 1, 3 * pairs, lanes), F32),
            pltpu.VMEM((3 * pairs, lanes), F32),
            pltpu.VMEM((n_d - 1, 3 * pairs, lanes), F32),
            pltpu.VMEM((2, lanes), F32),
            pltpu.VMEM((n_all - 1, 2, lanes), F32),
            dma((8,)),
            dma((n_r - 1,)), dma((n_r - 1,)),
            dma((n_d - 1,)), dma((n_d - 1,)),
            dma((n_d - 1,)), dma((n_d - 1,)),
            dma((n_all - 1,)), dma((n_all - 1,)),
        ],
        compiler_params=pltpu.CompilerParams(
            collective_id=0, has_side_effects=True, vmem_limit_bytes=room
        ),
    )(*[pltpu.with_memory_space_constraint(x, pltpu.HBM) for x in inputs])
    return forces, scalars[1, 0], scalars[0, 0]


def solution(mesh):
    in_specs = (
        P("dimer", "rep", None, None),
        P("dimer", "rep"),
        P("dimer", "rep"),
        P(None, ("dimer", "rep")),
        P("dimer", None),
        P("dimer", None),
    )
    out_specs = (P(None, ("dimer", "rep")), P(), P())
    return jax.shard_map(
        functools.partial(on_device, mesh.shape["dimer"], mesh.shape["rep"]),
        mesh=mesh, in_specs=in_specs, out_specs=out_specs, check_vma=False,
    )
```

```python
import functools

import jax
import jax.numpy as jnp
from jax import lax
from jax.experimental import pallas as pl
from jax.experimental.pallas import tpu as pltpu
from jax.sharding import PartitionSpec as P

MESH = pl.DeviceIdType.MESH
F32, BF16 = jnp.float32, jnp.bfloat16


def kernel(
    n_d, n_r, integ, *refs,
):
    smalls, (forces, scalars), (dens, eterm, pos, owner, local) = refs[:5], refs[5:7], refs[7:12]
    (
        ibuf, dbuf, in_a, acc, in_b, posb, in_p, sbuf, in_s,
        isem, a_send, a_recv, b_send, b_recv, p_send, p_recv, s_send, s_recv,
    ) = refs[12:]
    slots, terms = dens.shape
    lanes = ibuf.shape[3]
    half = lanes // 2
    pairs = pos.shape[1] // lanes
    per_rep = 2 * pairs
    n_all = n_d * n_r
    rows = n_r * n_d * pairs
    d, r = lax.axis_index("dimer"), lax.axis_index("rep")
    me = d * n_r + r

    def partner(step, mine, count):
        flip = (2 * mine) // count
        at = flip * step + (1 - flip) * (count - 2 - step)
        peer = at + (at + count - mine) // count
        return peer, mine - (mine + count - 1 - peer) // count

    def each(count, act):
        if count <= 64:
            for k in range(count - 1):
                act(k)
        else:
            lax.fori_loop(0, count - 1, lambda k, carry: (act(k), carry)[1], 0)

    loads = [pltpu.make_async_copy(integ.at[:, c], ibuf.at[c], isem.at[c]) for c in range(3)]
    fetches = [
        pltpu.make_async_copy(source, held, isem.at[3 + i])
        for i, (source, held) in enumerate(zip(smalls, (dens, eterm, pos, owner, local)))
    ]
    for copy in loads + fetches:
        copy.start()

    barrier = pltpu.get_barrier_semaphore()

    def greet(k):
        peer, _ = partner(k, me, n_all)
        pl.semaphore_signal(
            barrier, inc=1, device_id=(peer // n_r, lax.rem(peer, n_r)), device_id_type=MESH
        )

    each(n_all, greet)

    for fetch in fetches:
        fetch.wait()

    weights = dens[...].astype(F32)
    span = slots * terms
    lane = lax.broadcasted_iota(jnp.int32, (slots, span), 1)
    first = lax.broadcasted_iota(jnp.int32, (slots, span), 0) * terms
    spread = jnp.concatenate([weights] * slots, axis=1)
    diagonal = jnp.where((lane >= first) & (lane < first + terms), spread, 0.0).astype(BF16)

    name, index = owner[...], local[...]
    rep = jnp.zeros_like(index)
    for bound in range(1, n_r):
        rep = rep + (index >= bound * per_rep).astype(jnp.int32)
    rest = index - rep * per_rep
    target = rep * (n_d * pairs) + name * pairs + lax.shift_right_logical(rest, 1)
    parity = rest & 1
    keys = []
    for t in range(2):
        for h in range(2):
            keys.append(jnp.where(parity[t : t + 1] == h, target[t : t + 1], -1))
    key = jnp.concatenate(keys, axis=1)
    place = lax.broadcasted_iota(jnp.int32, (rows, 4 * slots), 0)
    hot = jnp.where(place == key, 1.0, 0.0).astype(BF16)
    hot = jnp.concatenate([hot] * 3, axis=1)

    for c in range(3):
        for j in range(pairs):
            posb[c * pairs + j : c * pairs + j + 1] = pos[c : c + 1, j * lanes : (j + 1) * lanes]
    energy = jnp.sum(weights * eterm[...].astype(F32), axis=0, keepdims=True)
    sbuf[1:2] = jnp.concatenate([energy, jnp.zeros((1, lanes - terms), F32)], axis=1)

    side = lax.broadcasted_iota(jnp.int32, (slots, lanes), 1) >= half
    for c in range(3):
        loads[c].wait()
        grad = jnp.dot(
            diagonal, ibuf[c].reshape(span, lanes), preferred_element_type=F32
        )
        swap = pltpu.roll(grad, half, 1)
        spreads = jnp.concatenate(
            [
                jnp.where(side, 0.0, grad),
                jnp.where(side, swap, 0.0),
                jnp.where(side, 0.0, swap),
                jnp.where(side, grad, 0.0),
            ],
            axis=0,
        )
        high = spreads.astype(BF16)
        left = spreads - high.astype(F32)
        middle = left.astype(BF16)
        low = (left - middle.astype(F32)).astype(BF16)
        placed = jnp.dot(
            hot, jnp.concatenate([high, middle, low], axis=0), preferred_element_type=F32
        )
        for q in range(n_r):
            dbuf[q, c] = placed[q * n_d * pairs : (q + 1) * n_d * pairs]

    pl.semaphore_wait(barrier, n_all - 1)

    a_copies = []
    for k in range(1, n_r):
        to = lax.rem(r + k, n_r)
        a_copies.append(
            pltpu.make_async_remote_copy(
                src_ref=dbuf.at[to], dst_ref=in_a.at[k - 1],
                send_sem=a_send.at[k - 1], recv_sem=a_recv.at[k - 1],
                device_id=(d, to), device_id_type=MESH,
            )
        )
    for copy in a_copies:
        copy.start()

    def over_dimer(k, source, held, send, recv):
        peer, slot = partner(k, d, n_d)
        return pltpu.make_async_remote_copy(
            src_ref=source(peer), dst_ref=held.at[slot],
            send_sem=send.at[k], recv_sem=recv.at[slot],
            device_id=(peer, r), device_id_type=MESH,
        )

    def arrived(k, held, recv):
        pltpu.make_async_copy(held.at[k], held.at[k], recv.at[k]).wait()

    def p_copy(k):
        return over_dimer(k, lambda peer: posb, in_p, p_send, p_recv)

    def b_copy(k):
        return over_dimer(k, lambda peer: acc.at[peer], in_b, b_send, b_recv)

    def s_copy(k):
        peer, slot = partner(k, me, n_all)
        return pltpu.make_async_remote_copy(
            src_ref=sbuf, dst_ref=in_s.at[slot],
            send_sem=s_send.at[k], recv_sem=s_recv.at[slot],
            device_id=(peer // n_r, lax.rem(peer, n_r)), device_id_type=MESH,
        )

    each(n_d, lambda k: p_copy(k).start())
    for copy in a_copies:
        copy.wait_recv()
    for c in range(3):
        total = dbuf[r, c]
        for k in range(n_r - 1):
            total = total + in_a[k, c]
        for o in range(n_d):
            acc[o, c * pairs : (c + 1) * pairs] = total[o * pairs : (o + 1) * pairs]
    each(n_d, lambda k: b_copy(k).start())
    each(n_d, lambda k: arrived(k, in_p, p_recv))

    def virial_of(k, carry):
        return carry + acc[k + (k + n_d - d) // n_d] * in_p[k]

    products = acc[d] * posb[...]
    if n_d <= 64:
        for k in range(n_d - 1):
            products = virial_of(k, products)
    else:
        products = lax.fori_loop(0, n_d - 1, virial_of, products)
    sbuf[0:1] = jnp.sum(products, axis=0, keepdims=True)
    each(n_all, lambda k: s_copy(k).start())

    for copy in a_copies:
        copy.wait_send()
    each(n_d, lambda k: p_copy(k).wait_send())
    each(n_d, lambda k: arrived(k, in_b, b_recv))
    total = acc[d] + jnp.sum(in_b[...], axis=0)
    for c in range(3):
        for j in range(pairs):
            forces[c : c + 1, j * lanes : (j + 1) * lanes] = total[c * pairs + j : c * pairs + j + 1]
    each(n_d, lambda k: b_copy(k).wait_send())
    each(n_all, lambda k: s_copy(k).wait_send())

    each(n_all, lambda k: arrived(k, in_s, s_recv))
    both = sbuf[...] + jnp.sum(in_s[...], axis=0)
    both = jnp.sum(both, axis=1, keepdims=True)
    row = lax.broadcasted_iota(jnp.int32, both.shape, 0)
    both = jnp.where(row == 0, both * (-1.0 / 3.0), both)
    scalars[...] = jnp.broadcast_to(both, scalars.shape)


def on_device(n_d, n_r, integrals, density, energy_terms, positions, owners, local):
    slots, terms, _, lanes = integrals.shape
    pairs = positions.shape[1] // lanes
    n_all = n_d * n_r
    room = 2 * (2 * integrals.size + 4 * lanes * 8 * n_d * n_r * (3 * pairs + 4)) + 2**21
    vmem = pl.BlockSpec(memory_space=pltpu.VMEM)
    dma = pltpu.SemaphoreType.DMA
    inputs = (
        jnp.transpose(integrals, (0, 2, 1, 3)), density, energy_terms, positions,
        owners.T, local.T,
    )
    forces, scalars = pl.pallas_call(
        functools.partial(kernel, n_d, n_r),
        out_shape=(
            jax.ShapeDtypeStruct(positions.shape, F32),
            jax.ShapeDtypeStruct((2, lanes), F32),
        ),
        in_specs=[pl.BlockSpec(memory_space=pltpu.HBM)] * 6,
        out_specs=(vmem, vmem),
        scratch_shapes=[
            pltpu.VMEM(density.shape, BF16),
            pltpu.VMEM(energy_terms.shape, BF16),
            pltpu.VMEM(positions.shape, F32),
            pltpu.VMEM((2, slots), jnp.int32),
            pltpu.VMEM((2, slots), jnp.int32),
            pltpu.VMEM((3, slots, terms, lanes), BF16),
            pltpu.VMEM((n_r, 3, n_d * pairs, lanes), F32),
            pltpu.VMEM((n_r - 1, 3, n_d * pairs, lanes), F32),
            pltpu.VMEM((n_d, 3 * pairs, lanes), F32),
            pltpu.VMEM((n_d - 1, 3 * pairs, lanes), F32),
            pltpu.VMEM((3 * pairs, lanes), F32),
            pltpu.VMEM((n_d - 1, 3 * pairs, lanes), F32),
            pltpu.VMEM((2, lanes), F32),
            pltpu.VMEM((n_all - 1, 2, lanes), F32),
            dma((8,)),
            dma((n_r - 1,)), dma((n_r - 1,)),
            dma((n_d - 1,)), dma((n_d - 1,)),
            dma((n_d - 1,)), dma((n_d - 1,)),
            dma((n_all - 1,)), dma((n_all - 1,)),
        ],
        compiler_params=pltpu.CompilerParams(
            collective_id=0, has_side_effects=True, vmem_limit_bytes=room
        ),
    )(*[pltpu.with_memory_space_constraint(x, pltpu.HBM) for x in inputs])
    return forces, scalars[1, 0], scalars[0, 0]


def solution(mesh):
    in_specs = (
        P("dimer", "rep", None, None),
        P("dimer", "rep"),
        P("dimer", "rep"),
        P(None, ("dimer", "rep")),
        P("dimer", None),
        P("dimer", None),
    )
    out_specs = (P(None, ("dimer", "rep")), P(), P())
    return jax.shard_map(
        functools.partial(on_device, mesh.shape["dimer"], mesh.shape["rep"]),
        mesh=mesh, in_specs=in_specs, out_specs=out_specs, check_vma=False,
    )
```

```python
import functools

import jax
import jax.numpy as jnp
from jax import lax
from jax.experimental import pallas as pl
from jax.experimental.pallas import tpu as pltpu
from jax.sharding import PartitionSpec as P

MESH = pl.DeviceIdType.MESH
F32, BF16 = jnp.float32, jnp.bfloat16


def kernel(
    n_d, n_r, integ, *refs,
):
    smalls, (forces, scalars), (dens, eterm, pos, owner, local) = refs[:5], refs[5:7], refs[7:12]
    (
        ibuf, dbuf, in_a, acc, in_b, posb, in_p, sbuf, in_s,
        isem, a_send, a_recv, b_send, b_recv, p_send, p_recv, s_send, s_recv,
    ) = refs[12:]
    slots, terms = dens.shape
    lanes = ibuf.shape[3]
    half = lanes // 2
    pairs = pos.shape[1] // lanes
    per_rep = 2 * pairs
    n_all = n_d * n_r
    rows = n_r * n_d * pairs
    d, r = lax.axis_index("dimer"), lax.axis_index("rep")
    me = d * n_r + r

    def partner(step, mine, count):
        flip = (2 * mine) // count
        at = flip * step + (1 - flip) * (count - 2 - step)
        peer = at + (at + count - mine) // count
        return peer, mine - (mine + count - 1 - peer) // count

    def each(count, act):
        if count <= 64:
            for k in range(count - 1):
                act(k)
        else:
            lax.fori_loop(0, count - 1, lambda k, carry: (act(k), carry)[1], 0)

    loads = [pltpu.make_async_copy(integ.at[:, c], ibuf.at[c], isem.at[c]) for c in range(3)]
    fetches = [
        pltpu.make_async_copy(source, held, isem.at[3 + i])
        for i, (source, held) in enumerate(zip(smalls, (dens, eterm, pos, owner, local)))
    ]
    for copy in loads + fetches:
        copy.start()

    barrier = pltpu.get_barrier_semaphore()

    def greet(*device):
        pl.semaphore_signal(barrier, inc=1, device_id=device, device_id_type=MESH)

    each(n_d, lambda k: greet(partner(k, d, n_d)[0], r))
    each(n_r, lambda k: greet(d, partner(k, r, n_r)[0]))

    for fetch in fetches:
        fetch.wait()

    weights = dens[...].astype(F32)
    span = slots * terms
    lane = lax.broadcasted_iota(jnp.int32, (slots, span), 1)
    first = lax.broadcasted_iota(jnp.int32, (slots, span), 0) * terms
    spread = jnp.concatenate([weights] * slots, axis=1)
    diagonal = jnp.where((lane >= first) & (lane < first + terms), spread, 0.0).astype(BF16)

    name, index = owner[...], local[...]
    rep = jnp.zeros_like(index)
    for bound in range(1, n_r):
        rep = rep + (index >= bound * per_rep).astype(jnp.int32)
    rest = index - rep * per_rep
    target = rep * (n_d * pairs) + name * pairs + lax.shift_right_logical(rest, 1)
    parity = rest & 1
    keys = []
    for t in range(2):
        for h in range(2):
            keys.append(jnp.where(parity[t : t + 1] == h, target[t : t + 1], -1))
    key = jnp.concatenate(keys, axis=1)
    place = lax.broadcasted_iota(jnp.int32, (rows, 4 * slots), 0)
    hot = jnp.where(place == key, 1.0, 0.0).astype(BF16)
    hot = jnp.concatenate([hot] * 3, axis=1)

    for c in range(3):
        for j in range(pairs):
            posb[c * pairs + j : c * pairs + j + 1] = pos[c : c + 1, j * lanes : (j + 1) * lanes]
    energy = jnp.sum(weights * eterm[...].astype(F32), axis=0, keepdims=True)
    sbuf[1:2] = jnp.concatenate([energy, jnp.zeros((1, lanes - terms), F32)], axis=1)

    side = lax.broadcasted_iota(jnp.int32, (slots, lanes), 1) >= half
    for c in range(3):
        loads[c].wait()
        grad = jnp.dot(
            diagonal, ibuf[c].reshape(span, lanes), preferred_element_type=F32
        )
        swap = pltpu.roll(grad, half, 1)
        spreads = jnp.concatenate(
            [
                jnp.where(side, 0.0, grad),
                jnp.where(side, swap, 0.0),
                jnp.where(side, 0.0, swap),
                jnp.where(side, grad, 0.0),
            ],
            axis=0,
        )
        high = spreads.astype(BF16)
        left = spreads - high.astype(F32)
        middle = left.astype(BF16)
        low = (left - middle.astype(F32)).astype(BF16)
        placed = jnp.dot(
            hot, jnp.concatenate([high, middle, low], axis=0), preferred_element_type=F32
        )
        for q in range(n_r):
            dbuf[q, c] = placed[q * n_d * pairs : (q + 1) * n_d * pairs]

    pl.semaphore_wait(barrier, n_d + n_r - 2)

    a_copies = []
    for k in range(1, n_r):
        to = lax.rem(r + k, n_r)
        a_copies.append(
            pltpu.make_async_remote_copy(
                src_ref=dbuf.at[to], dst_ref=in_a.at[k - 1],
                send_sem=a_send.at[k - 1], recv_sem=a_recv.at[k - 1],
                device_id=(d, to), device_id_type=MESH,
            )
        )

    def over_dimer(k, source, held, send, recv):
        peer, slot = partner(k, d, n_d)
        return pltpu.make_async_remote_copy(
            src_ref=source(peer), dst_ref=held.at[slot],
            send_sem=send.at[k], recv_sem=recv.at[slot],
            device_id=(peer, r), device_id_type=MESH,
        )

    def arrived(k, held, recv):
        pltpu.make_async_copy(held.at[k], held.at[k], recv.at[k]).wait()

    def p_copy(k):
        return over_dimer(k, lambda peer: posb, in_p, p_send, p_recv)

    def b_copy(k):
        return over_dimer(k, lambda peer: acc.at[peer], in_b, b_send, b_recv)

    def s_copy(k):
        peer, slot = partner(k, me, n_all)
        return pltpu.make_async_remote_copy(
            src_ref=sbuf, dst_ref=in_s.at[slot],
            send_sem=s_send.at[k], recv_sem=s_recv.at[slot],
            device_id=(peer // n_r, lax.rem(peer, n_r)), device_id_type=MESH,
        )

    each(n_d, lambda k: p_copy(k).start())
    for copy in a_copies:
        copy.start()
    for copy in a_copies:
        copy.wait_recv()
    for c in range(3):
        total = dbuf[r, c]
        for k in range(n_r - 1):
            total = total + in_a[k, c]
        for o in range(n_d):
            acc[o, c * pairs : (c + 1) * pairs] = total[o * pairs : (o + 1) * pairs]
    each(n_d, lambda k: b_copy(k).start())
    each(n_d, lambda k: arrived(k, in_p, p_recv))

    def virial_of(k, carry):
        return carry + acc[k + (k + n_d - d) // n_d] * in_p[k]

    products = acc[d] * posb[...]
    if n_d <= 64:
        for k in range(n_d - 1):
            products = virial_of(k, products)
    else:
        products = lax.fori_loop(0, n_d - 1, virial_of, products)
    sbuf[0:1] = jnp.sum(products, axis=0, keepdims=True)
    each(n_all, lambda k: s_copy(k).start())

    for copy in a_copies:
        copy.wait_send()
    each(n_d, lambda k: p_copy(k).wait_send())
    each(n_d, lambda k: arrived(k, in_b, b_recv))
    total = acc[d] + jnp.sum(in_b[...], axis=0)
    for c in range(3):
        for j in range(pairs):
            forces[c : c + 1, j * lanes : (j + 1) * lanes] = total[c * pairs + j : c * pairs + j + 1]
    each(n_d, lambda k: b_copy(k).wait_send())
    each(n_all, lambda k: s_copy(k).wait_send())

    each(n_all, lambda k: arrived(k, in_s, s_recv))
    both = sbuf[...] + jnp.sum(in_s[...], axis=0)
    both = jnp.sum(both, axis=1, keepdims=True)
    row = lax.broadcasted_iota(jnp.int32, both.shape, 0)
    both = jnp.where(row == 0, both * (-1.0 / 3.0), both)
    scalars[...] = jnp.broadcast_to(both, scalars.shape)


def on_device(n_d, n_r, integrals, density, energy_terms, positions, owners, local):
    slots, terms, _, lanes = integrals.shape
    pairs = positions.shape[1] // lanes
    n_all = n_d * n_r
    room = 2 * (2 * integrals.size + 4 * lanes * 8 * n_d * n_r * (3 * pairs + 4)) + 2**21
    vmem = pl.BlockSpec(memory_space=pltpu.VMEM)
    dma = pltpu.SemaphoreType.DMA
    inputs = (
        jnp.transpose(integrals, (0, 2, 1, 3)), density, energy_terms, positions,
        owners.T, local.T,
    )
    forces, scalars = pl.pallas_call(
        functools.partial(kernel, n_d, n_r),
        out_shape=(
            jax.ShapeDtypeStruct(positions.shape, F32),
            jax.ShapeDtypeStruct((2, lanes), F32),
        ),
        in_specs=[pl.BlockSpec(memory_space=pltpu.HBM)] * 6,
        out_specs=(vmem, vmem),
        scratch_shapes=[
            pltpu.VMEM(density.shape, BF16),
            pltpu.VMEM(energy_terms.shape, BF16),
            pltpu.VMEM(positions.shape, F32),
            pltpu.VMEM((2, slots), jnp.int32),
            pltpu.VMEM((2, slots), jnp.int32),
            pltpu.VMEM((3, slots, terms, lanes), BF16),
            pltpu.VMEM((n_r, 3, n_d * pairs, lanes), F32),
            pltpu.VMEM((n_r - 1, 3, n_d * pairs, lanes), F32),
            pltpu.VMEM((n_d, 3 * pairs, lanes), F32),
            pltpu.VMEM((n_d - 1, 3 * pairs, lanes), F32),
            pltpu.VMEM((3 * pairs, lanes), F32),
            pltpu.VMEM((n_d - 1, 3 * pairs, lanes), F32),
            pltpu.VMEM((2, lanes), F32),
            pltpu.VMEM((n_all - 1, 2, lanes), F32),
            dma((8,)),
            dma((n_r - 1,)), dma((n_r - 1,)),
            dma((n_d - 1,)), dma((n_d - 1,)),
            dma((n_d - 1,)), dma((n_d - 1,)),
            dma((n_all - 1,)), dma((n_all - 1,)),
        ],
        compiler_params=pltpu.CompilerParams(
            collective_id=0, has_side_effects=True, vmem_limit_bytes=room
        ),
    )(*[pltpu.with_memory_space_constraint(x, pltpu.HBM) for x in inputs])
    return forces, scalars[1, 0], scalars[0, 0]


def solution(mesh):
    in_specs = (
        P("dimer", "rep", None, None),
        P("dimer", "rep"),
        P("dimer", "rep"),
        P(None, ("dimer", "rep")),
        P("dimer", None),
        P("dimer", None),
    )
    out_specs = (P(None, ("dimer", "rep")), P(), P())
    return jax.shard_map(
        functools.partial(on_device, mesh.shape["dimer"], mesh.shape["rep"]),
        mesh=mesh, in_specs=in_specs, out_specs=out_specs, check_vma=False,
    )
```

```python
import functools

import jax
import jax.numpy as jnp
from jax import lax
from jax.experimental import pallas as pl
from jax.experimental.pallas import tpu as pltpu
from jax.sharding import PartitionSpec as P

MESH = pl.DeviceIdType.MESH
F32, BF16 = jnp.float32, jnp.bfloat16


def kernel(
    n_d, n_r, integ, *refs,
):
    smalls, (forces, scalars), (dens, eterm, pos, owner, local) = refs[:5], refs[5:7], refs[7:12]
    (
        ibuf, dbuf, in_a, acc, in_b, posb, in_p, sbuf, in_s,
        isem, a_send, a_recv, b_send, b_recv, p_send, p_recv, s_send, s_recv,
    ) = refs[12:]
    slots, terms = dens.shape
    lanes = ibuf.shape[3]
    half = lanes // 2
    pairs = pos.shape[1] // lanes
    per_rep = 2 * pairs
    n_all = n_d * n_r
    rows = n_r * n_d * pairs
    d, r = lax.axis_index("dimer"), lax.axis_index("rep")
    me = d * n_r + r

    def partner(step, mine, count):
        flip = (2 * mine) // count
        at = flip * step + (1 - flip) * (count - 2 - step)
        peer = at + (at + count - mine) // count
        return peer, mine - (mine + count - 1 - peer) // count

    def each(count, act):
        if count <= 64:
            for k in range(count - 1):
                act(k)
        else:
            lax.fori_loop(0, count - 1, lambda k, carry: (act(k), carry)[1], 0)

    loads = [pltpu.make_async_copy(integ.at[:, c], ibuf.at[c], isem.at[c]) for c in range(3)]
    fetches = [
        pltpu.make_async_copy(source, held, isem.at[3 + i])
        for i, (source, held) in enumerate(zip(smalls, (dens, eterm, pos, owner, local)))
    ]
    for copy in loads + fetches:
        copy.start()

    barrier = pltpu.get_barrier_semaphore()

    def greet(*device):
        pl.semaphore_signal(barrier, inc=1, device_id=device, device_id_type=MESH)

    each(n_d, lambda k: greet(partner(k, d, n_d)[0], r))
    each(n_r, lambda k: greet(d, partner(k, r, n_r)[0]))

    for fetch in fetches:
        fetch.wait()

    weights = dens[...].astype(F32)
    span = slots * terms
    lane = lax.broadcasted_iota(jnp.int32, (slots, span), 1)
    first = lax.broadcasted_iota(jnp.int32, (slots, span), 0) * terms
    spread = jnp.concatenate([weights] * slots, axis=1)
    diagonal = jnp.where((lane >= first) & (lane < first + terms), spread, 0.0).astype(BF16)

    name, index = owner[...], local[...]
    rep = jnp.zeros_like(index)
    for bound in range(1, n_r):
        rep = rep + (index >= bound * per_rep).astype(jnp.int32)
    rest = index - rep * per_rep
    target = rep * (n_d * pairs) + name * pairs + lax.shift_right_logical(rest, 1)
    parity = rest & 1
    keys = []
    for t in range(2):
        for h in range(2):
            keys.append(jnp.where(parity[t : t + 1] == h, target[t : t + 1], -1))
    key = jnp.concatenate(keys, axis=1)
    place = lax.broadcasted_iota(jnp.int32, (rows, 4 * slots), 0)
    hot = jnp.where(place == key, 1.0, 0.0).astype(BF16)
    hot = jnp.concatenate([hot] * 3, axis=1)

    for c in range(3):
        for j in range(pairs):
            posb[c * pairs + j : c * pairs + j + 1] = pos[c : c + 1, j * lanes : (j + 1) * lanes]
    energy = jnp.sum(weights * eterm[...].astype(F32), axis=0, keepdims=True)
    sbuf[1:2] = jnp.concatenate([energy, jnp.zeros((1, lanes - terms), F32)], axis=1)

    side = lax.broadcasted_iota(jnp.int32, (slots, lanes), 1) >= half
    for c in range(3):
        loads[c].wait()
        grad = jnp.dot(
            diagonal, ibuf[c].reshape(span, lanes), preferred_element_type=F32
        )
        swap = pltpu.roll(grad, half, 1)
        spreads = jnp.concatenate(
            [
                jnp.where(side, 0.0, grad),
                jnp.where(side, swap, 0.0),
                jnp.where(side, 0.0, swap),
                jnp.where(side, grad, 0.0),
            ],
            axis=0,
        )
        high = spreads.astype(BF16)
        left = spreads - high.astype(F32)
        middle = left.astype(BF16)
        low = (left - middle.astype(F32)).astype(BF16)
        placed = jnp.dot(
            hot, jnp.concatenate([high, middle, low], axis=0), preferred_element_type=F32
        )
        for q in range(n_r):
            dbuf[q, c] = placed[q * n_d * pairs : (q + 1) * n_d * pairs]

    pl.semaphore_wait(barrier, n_d + n_r - 2)

    a_copies = []
    for k in range(1, n_r):
        to = lax.rem(r + k, n_r)
        a_copies.append(
            pltpu.make_async_remote_copy(
                src_ref=dbuf.at[to], dst_ref=in_a.at[k - 1],
                send_sem=a_send.at[k - 1], recv_sem=a_recv.at[k - 1],
                device_id=(d, to), device_id_type=MESH,
            )
        )

    def over_dimer(k, source, held, send, recv):
        peer, slot = partner(k, d, n_d)
        return pltpu.make_async_remote_copy(
            src_ref=source(peer), dst_ref=held.at[slot],
            send_sem=send, recv_sem=recv,
            device_id=(peer, r), device_id_type=MESH,
        )

    def all_of(held, semaphore):
        pltpu.make_async_copy(held, held, semaphore).wait()

    def p_copy(k):
        return over_dimer(k, lambda peer: posb, in_p, p_send, p_recv)

    def b_copy(k):
        return over_dimer(k, lambda peer: acc.at[peer], in_b, b_send, b_recv)

    def s_copy(k):
        peer, slot = partner(k, me, n_all)
        return pltpu.make_async_remote_copy(
            src_ref=sbuf, dst_ref=in_s.at[slot],
            send_sem=s_send, recv_sem=s_recv,
            device_id=(peer // n_r, lax.rem(peer, n_r)), device_id_type=MESH,
        )

    each(n_d, lambda k: p_copy(k).start())
    for copy in a_copies:
        copy.start()
    for copy in a_copies:
        copy.wait_recv()
    for c in range(3):
        total = dbuf[r, c]
        for k in range(n_r - 1):
            total = total + in_a[k, c]
        for o in range(n_d):
            acc[o, c * pairs : (c + 1) * pairs] = total[o * pairs : (o + 1) * pairs]
    each(n_d, lambda k: b_copy(k).start())
    all_of(in_p, p_recv)

    def virial_of(k, carry):
        return carry + acc[k + (k + n_d - d) // n_d] * in_p[k]

    products = acc[d] * posb[...]
    if n_d <= 64:
        for k in range(n_d - 1):
            products = virial_of(k, products)
    else:
        products = lax.fori_loop(0, n_d - 1, virial_of, products)
    sbuf[0:1] = jnp.sum(products, axis=0, keepdims=True)
    each(n_all, lambda k: s_copy(k).start())

    for copy in a_copies:
        copy.wait_send()
    all_of(in_p, p_send)
    all_of(in_b, b_recv)
    total = acc[d] + jnp.sum(in_b[...], axis=0)
    for c in range(3):
        for j in range(pairs):
            forces[c : c + 1, j * lanes : (j + 1) * lanes] = total[c * pairs + j : c * pairs + j + 1]
    all_of(in_b, b_send)
    all_of(in_s, s_send)

    all_of(in_s, s_recv)
    both = sbuf[...] + jnp.sum(in_s[...], axis=0)
    both = jnp.sum(both, axis=1, keepdims=True)
    row = lax.broadcasted_iota(jnp.int32, both.shape, 0)
    both = jnp.where(row == 0, both * (-1.0 / 3.0), both)
    scalars[...] = jnp.broadcast_to(both, scalars.shape)


def on_device(n_d, n_r, integrals, density, energy_terms, positions, owners, local):
    slots, terms, _, lanes = integrals.shape
    pairs = positions.shape[1] // lanes
    n_all = n_d * n_r
    room = 2 * (2 * integrals.size + 4 * lanes * 8 * n_d * n_r * (3 * pairs + 4)) + 2**21
    vmem = pl.BlockSpec(memory_space=pltpu.VMEM)
    dma = pltpu.SemaphoreType.DMA
    inputs = (
        jnp.transpose(integrals, (0, 2, 1, 3)), density, energy_terms, positions,
        owners.T, local.T,
    )
    forces, scalars = pl.pallas_call(
        functools.partial(kernel, n_d, n_r),
        out_shape=(
            jax.ShapeDtypeStruct(positions.shape, F32),
            jax.ShapeDtypeStruct((2, lanes), F32),
        ),
        in_specs=[pl.BlockSpec(memory_space=pltpu.HBM)] * 6,
        out_specs=(vmem, vmem),
        scratch_shapes=[
            pltpu.VMEM(density.shape, BF16),
            pltpu.VMEM(energy_terms.shape, BF16),
            pltpu.VMEM(positions.shape, F32),
            pltpu.VMEM((2, slots), jnp.int32),
            pltpu.VMEM((2, slots), jnp.int32),
            pltpu.VMEM((3, slots, terms, lanes), BF16),
            pltpu.VMEM((n_r, 3, n_d * pairs, lanes), F32),
            pltpu.VMEM((n_r - 1, 3, n_d * pairs, lanes), F32),
            pltpu.VMEM((n_d, 3 * pairs, lanes), F32),
            pltpu.VMEM((n_d - 1, 3 * pairs, lanes), F32),
            pltpu.VMEM((3 * pairs, lanes), F32),
            pltpu.VMEM((n_d - 1, 3 * pairs, lanes), F32),
            pltpu.VMEM((2, lanes), F32),
            pltpu.VMEM((n_all - 1, 2, lanes), F32),
            dma((8,)),
            dma((n_r - 1,)), dma((n_r - 1,)),
            dma, dma, dma, dma, dma, dma,
        ],
        compiler_params=pltpu.CompilerParams(
            collective_id=0, has_side_effects=True, vmem_limit_bytes=room
        ),
    )(*[pltpu.with_memory_space_constraint(x, pltpu.HBM) for x in inputs])
    return forces, scalars[1, 0], scalars[0, 0]


def solution(mesh):
    in_specs = (
        P("dimer", "rep", None, None),
        P("dimer", "rep"),
        P("dimer", "rep"),
        P(None, ("dimer", "rep")),
        P("dimer", None),
        P("dimer", None),
    )
    out_specs = (P(None, ("dimer", "rep")), P(), P())
    return jax.shard_map(
        functools.partial(on_device, mesh.shape["dimer"], mesh.shape["rep"]),
        mesh=mesh, in_specs=in_specs, out_specs=out_specs, check_vma=False,
    )
```

```python
import functools

import jax
import jax.numpy as jnp
from jax import lax
from jax.experimental import pallas as pl
from jax.experimental.pallas import tpu as pltpu
from jax.sharding import PartitionSpec as P

MESH = pl.DeviceIdType.MESH
F32, BF16 = jnp.float32, jnp.bfloat16


def kernel(
    n_d, n_r, integ, *refs,
):
    smalls, (forces, scalars), (dens, eterm, pos, owner, local) = refs[:5], refs[5:7], refs[7:12]
    (
        ibuf, dbuf, in_a, acc, in_b, posb, in_p, sbuf, in_s,
        isem, a_send, a_recv, b_send, b_recv, p_send, p_recv, s_send, s_recv,
    ) = refs[12:]
    slots, terms = dens.shape
    lanes = ibuf.shape[3]
    half = lanes // 2
    pairs = pos.shape[1] // lanes
    per_rep = 2 * pairs
    n_all = n_d * n_r
    rows = n_r * n_d * pairs
    d, r = lax.axis_index("dimer"), lax.axis_index("rep")
    me = d * n_r + r

    def partner(step, mine, count):
        flip = lax.div(2 * mine, count)
        at = flip * step + (1 - flip) * (count - 2 - step)
        peer = at + lax.div(at + count - mine, count)
        return peer, mine - lax.div(mine + count - 1 - peer, count)

    def over(peer):
        row = lax.div(peer, n_r)
        return row, peer - row * n_r

    def each(count, act):
        if count <= 64:
            for k in range(count - 1):
                act(k)
        else:
            lax.fori_loop(0, count - 1, lambda k, carry: (act(k), carry)[1], 0)

    loads = [pltpu.make_async_copy(integ.at[:, c], ibuf.at[c], isem.at[c]) for c in range(3)]
    fetches = [
        pltpu.make_async_copy(source, held, isem.at[3 + i])
        for i, (source, held) in enumerate(zip(smalls, (dens, eterm, pos, owner, local)))
    ]
    for copy in loads + fetches:
        copy.start()

    barrier = pltpu.get_barrier_semaphore()

    def greet(*device):
        pl.semaphore_signal(barrier, inc=1, device_id=device, device_id_type=MESH)

    each(n_d, lambda k: greet(partner(k, d, n_d)[0], r))
    each(n_r, lambda k: greet(d, partner(k, r, n_r)[0]))

    for fetch in fetches:
        fetch.wait()

    weights = dens[...].astype(F32)
    span = slots * terms
    lane = lax.broadcasted_iota(jnp.int32, (slots, span), 1)
    first = lax.broadcasted_iota(jnp.int32, (slots, span), 0) * terms
    spread = jnp.concatenate([weights] * slots, axis=1)
    diagonal = jnp.where((lane >= first) & (lane < first + terms), spread, 0.0).astype(BF16)

    name, index = owner[...], local[...]
    rep = jnp.zeros_like(index)
    for bound in range(1, n_r):
        rep = rep + (index >= bound * per_rep).astype(jnp.int32)
    rest = index - rep * per_rep
    target = rep * (n_d * pairs) + name * pairs + lax.shift_right_logical(rest, 1)
    parity = rest & 1
    keys = []
    for t in range(2):
        for h in range(2):
            keys.append(jnp.where(parity[t : t + 1] == h, target[t : t + 1], -1))
    key = jnp.concatenate(keys, axis=1)
    place = lax.broadcasted_iota(jnp.int32, (rows, 4 * slots), 0)
    hot = jnp.where(place == key, 1.0, 0.0).astype(BF16)
    hot = jnp.concatenate([hot] * 3, axis=1)

    for c in range(3):
        for j in range(pairs):
            posb[c * pairs + j : c * pairs + j + 1] = pos[c : c + 1, j * lanes : (j + 1) * lanes]
    energy = jnp.sum(weights * eterm[...].astype(F32), axis=0, keepdims=True)
    sbuf[1:2] = jnp.concatenate([energy, jnp.zeros((1, lanes - terms), F32)], axis=1)

    side = lax.broadcasted_iota(jnp.int32, (slots, lanes), 1) >= half
    for c in range(3):
        loads[c].wait()
        grad = jnp.dot(
            diagonal, ibuf[c].reshape(span, lanes), preferred_element_type=F32
        )
        swap = pltpu.roll(grad, half, 1)
        spreads = jnp.concatenate(
            [
                jnp.where(side, 0.0, grad),
                jnp.where(side, swap, 0.0),
                jnp.where(side, 0.0, swap),
                jnp.where(side, grad, 0.0),
            ],
            axis=0,
        )
        high = spreads.astype(BF16)
        left = spreads - high.astype(F32)
        middle = left.astype(BF16)
        low = (left - middle.astype(F32)).astype(BF16)
        placed = jnp.dot(
            hot, jnp.concatenate([high, middle, low], axis=0), preferred_element_type=F32
        )
        for q in range(n_r):
            dbuf[q, c] = placed[q * n_d * pairs : (q + 1) * n_d * pairs]

    pl.semaphore_wait(barrier, n_d + n_r - 2)

    a_copies = []
    for k in range(1, n_r):
        to = lax.rem(r + k, n_r)
        a_copies.append(
            pltpu.make_async_remote_copy(
                src_ref=dbuf.at[to], dst_ref=in_a.at[k - 1],
                send_sem=a_send, recv_sem=a_recv,
                device_id=(d, to), device_id_type=MESH,
            )
        )

    def over_dimer(k, source, held, send, recv):
        peer, slot = partner(k, d, n_d)
        return pltpu.make_async_remote_copy(
            src_ref=source(peer), dst_ref=held.at[slot],
            send_sem=send, recv_sem=recv,
            device_id=(peer, r), device_id_type=MESH,
        )

    def all_of(held, semaphore):
        pltpu.make_async_copy(held, held, semaphore).wait()

    def p_copy(k):
        return over_dimer(k, lambda peer: posb, in_p, p_send, p_recv)

    def b_copy(k):
        return over_dimer(k, lambda peer: acc.at[peer], in_b, b_send, b_recv)

    def s_copy(k):
        peer, slot = partner(k, me, n_all)
        return pltpu.make_async_remote_copy(
            src_ref=sbuf, dst_ref=in_s.at[slot],
            send_sem=s_send, recv_sem=s_recv,
            device_id=over(peer), device_id_type=MESH,
        )

    each(n_d, lambda k: p_copy(k).start())
    for copy in a_copies:
        copy.start()
    all_of(in_a, a_recv)
    for c in range(3):
        total = dbuf[r, c]
        for k in range(n_r - 1):
            total = total + in_a[k, c]
        for o in range(n_d):
            acc[o, c * pairs : (c + 1) * pairs] = total[o * pairs : (o + 1) * pairs]
    each(n_d, lambda k: b_copy(k).start())
    all_of(in_p, p_recv)

    def virial_of(k, carry):
        return carry + acc[k + lax.div(k + n_d - d, n_d)] * in_p[k]

    products = acc[d] * posb[...]
    if n_d <= 64:
        for k in range(n_d - 1):
            products = virial_of(k, products)
    else:
        products = lax.fori_loop(0, n_d - 1, virial_of, products)
    sbuf[0:1] = jnp.sum(products, axis=0, keepdims=True)
    each(n_all, lambda k: s_copy(k).start())

    all_of(in_a, a_send)
    all_of(in_p, p_send)
    all_of(in_b, b_recv)
    total = acc[d] + jnp.sum(in_b[...], axis=0)
    for c in range(3):
        for j in range(pairs):
            forces[c : c + 1, j * lanes : (j + 1) * lanes] = total[c * pairs + j : c * pairs + j + 1]
    all_of(in_b, b_send)
    all_of(in_s, s_send)

    all_of(in_s, s_recv)
    both = sbuf[...] + jnp.sum(in_s[...], axis=0)
    both = jnp.sum(both, axis=1, keepdims=True)
    row = lax.broadcasted_iota(jnp.int32, both.shape, 0)
    both = jnp.where(row == 0, both * (-1.0 / 3.0), both)
    scalars[...] = jnp.broadcast_to(both, scalars.shape)


def on_device(n_d, n_r, integrals, density, energy_terms, positions, owners, local):
    slots, terms, _, lanes = integrals.shape
    pairs = positions.shape[1] // lanes
    n_all = n_d * n_r
    room = 2 * (2 * integrals.size + 4 * lanes * 8 * n_d * n_r * (3 * pairs + 4)) + 2**21
    vmem = pl.BlockSpec(memory_space=pltpu.VMEM)
    dma = pltpu.SemaphoreType.DMA
    inputs = (
        jnp.transpose(integrals, (0, 2, 1, 3)), density, energy_terms, positions,
        owners.T, local.T,
    )
    forces, scalars = pl.pallas_call(
        functools.partial(kernel, n_d, n_r),
        out_shape=(
            jax.ShapeDtypeStruct(positions.shape, F32),
            jax.ShapeDtypeStruct((2, lanes), F32),
        ),
        in_specs=[pl.BlockSpec(memory_space=pltpu.HBM)] * 6,
        out_specs=(vmem, vmem),
        scratch_shapes=[
            pltpu.VMEM(density.shape, BF16),
            pltpu.VMEM(energy_terms.shape, BF16),
            pltpu.VMEM(positions.shape, F32),
            pltpu.VMEM((2, slots), jnp.int32),
            pltpu.VMEM((2, slots), jnp.int32),
            pltpu.VMEM((3, slots, terms, lanes), BF16),
            pltpu.VMEM((n_r, 3, n_d * pairs, lanes), F32),
            pltpu.VMEM((n_r - 1, 3, n_d * pairs, lanes), F32),
            pltpu.VMEM((n_d, 3 * pairs, lanes), F32),
            pltpu.VMEM((n_d - 1, 3 * pairs, lanes), F32),
            pltpu.VMEM((3 * pairs, lanes), F32),
            pltpu.VMEM((n_d - 1, 3 * pairs, lanes), F32),
            pltpu.VMEM((2, lanes), F32),
            pltpu.VMEM((n_all - 1, 2, lanes), F32),
            dma((8,)),
            dma, dma, dma, dma, dma, dma, dma, dma,
        ],
        compiler_params=pltpu.CompilerParams(
            collective_id=0, has_side_effects=True, vmem_limit_bytes=room
        ),
    )(*[pltpu.with_memory_space_constraint(x, pltpu.HBM) for x in inputs])
    return forces, scalars[1, 0], scalars[0, 0]


def solution(mesh):
    in_specs = (
        P("dimer", "rep", None, None),
        P("dimer", "rep"),
        P("dimer", "rep"),
        P(None, ("dimer", "rep")),
        P("dimer", None),
        P("dimer", None),
    )
    out_specs = (P(None, ("dimer", "rep")), P(), P())
    return jax.shard_map(
        functools.partial(on_device, mesh.shape["dimer"], mesh.shape["rep"]),
        mesh=mesh, in_specs=in_specs, out_specs=out_specs, check_vma=False,
    )
```
